32 devices in a mesh: rep: 1 (over z), r: 4 (over y), s: 8 (over x, core).
Axes of the slice: x: 4, y: 4, z: 1, core: 2. Of those that a mesh axis runs over, the one named last changes fastest.
The devices are a block of a 4x4x8 slice.
Arguments:
- x: bfloat16 [32, 2048, 1024], P(('rep', 'r', 's'))
- dy: bfloat16 [32, 2048, 1024], P(('rep', 'r', 's'))
- w_gate: bfloat16 [2, 1024, 2560], P(None, 's')
- w_up: bfloat16 [2, 1024, 2560], P(None, 's')
- w_down: bfloat16 [2, 2560, 1024], P(None, 's')
Outputs:
- output 1: bfloat16 [32, 2048, 1024], P(('rep', 'r', 's'))
- output 2: bfloat16 [2, 1024, 2560], P('rep', 's')
- output 3: bfloat16 [2, 1024, 2560], P('rep', 's')
- output 4: bfloat16 [2, 2560, 1024], P('rep', 's')
All inputs are finite; a program needn't handle non-finite values.
Results may differ from the reference program's by a relative error of at most 0.018.
Values are sent between devices in bfloat16 or wider.
A program may use at most 768 MiB of HBM per device.

```python
import jax
import jax.numpy as jnp
from jax import lax

SEQUENCES = 32
TOKENS = 2048
D = 1024
FF = 2560
LAYERS = 2
NAMES = ("w_gate", "w_up", "w_down")
SHAPES = {"w_gate": (LAYERS, D, FF), "w_up": (LAYERS, D, FF), "w_down": (LAYERS, FF, D)}


def bump(key, n, height):
    away = (jnp.arange(n, dtype=jnp.int32) - jax.random.randint(key, (), 0, n, jnp.int32)) % n
    return jnp.where(away < n // 8, height, 1.0)


def together(key, own, strength):
    shared = jax.random.normal(key, own.shape[1:], jnp.float32)
    return (own + strength * shared) * lax.rsqrt(1 + strength * strength)


def setup_inputs(seed: int = 0, part: int = 0) -> dict:
    kx, kdy, ka, kb, kz, kf, kh, kl, *kw = jax.random.split(jax.random.key(seed), 8 + len(NAMES))
    kx, kdy, ka, kb = (jax.random.fold_in(k, part) for k in (kx, kdy, ka, kb))
    shape = (SEQUENCES, TOKENS, D)
    much_x, much_dy = jax.random.uniform(kz, (2,), jnp.float32, 0.0, 1.0)
    layers = 2.0 ** jax.random.uniform(kl, (LAYERS, 1, 1), jnp.float32, -1.0, 1.0)
    x = together(ka, jax.random.normal(kx, shape, jnp.float32), much_x) * bump(kf, D, 4.0)
    dy = together(kb, jax.random.normal(kdy, shape, jnp.float32), much_dy)
    drawn = {"x": x.astype(jnp.bfloat16), "dy": (dy * (SEQUENCES * TOKENS) ** -0.5).astype(jnp.bfloat16)}
    for key, name in zip(kw, NAMES, strict=True):
        w = jax.random.normal(key, SHAPES[name], jnp.float32) * SHAPES[name][1] ** -0.5
        drawn[name] = (w * {"w_gate": 1.0, "w_up": bump(kh, FF, 4.0), "w_down": layers}[name]).astype(jnp.bfloat16)
    return drawn


def matmul(a, w):
    return jnp.dot(a, w, preferred_element_type=jnp.float32).astype(jnp.bfloat16)


def normed(h):
    wide = h.astype(jnp.float32)
    scale = lax.rsqrt(jnp.mean(wide**2, -1, keepdims=True) + 1e-6)
    return (wide * scale).astype(jnp.bfloat16)


def layer(h, w):
    a = normed(h)
    gate = jnp.dot(a, w["w_gate"], preferred_element_type=jnp.float32)
    up = jnp.dot(a, w["w_up"], preferred_element_type=jnp.float32)
    return h + matmul((jax.nn.silu(gate) * up).astype(jnp.bfloat16), w["w_down"])


def stack(weights, h):
    return lax.scan(lambda h, w: (layer(h, w), None), h, weights)[0]


def reference(x, dy, w_gate, w_up, w_down):
    weights = dict(zip(NAMES, (w_gate, w_up, w_down), strict=True))

    def take(so_far, sequence):
        h, by_y = sequence
        _, back = jax.vjp(stack, weights, h)
        by_weights, by_h = back(by_y)
        return jax.tree.map(lambda total, term: total + term.astype(jnp.float32), so_far, by_weights), by_h

    none_yet = {name: jnp.zeros(w.shape, jnp.float32) for name, w in weights.items()}
    by_weights, by_x = lax.scan(take, none_yet, (x, dy))
    return (by_x, *(by_weights[name].astype(jnp.bfloat16) for name in NAMES))
```

```python
import jax
import jax.numpy as jnp
from jax import lax
from jax.experimental import pallas as pl
from jax.experimental.pallas import tpu as pltpu
from jax.sharding import PartitionSpec as P

bf16, f32 = jnp.bfloat16, jnp.float32
NT = (((1,), (1,)), ((), ()))
EPS = 1e-6
WIDE = 512
VMEM = 64 * 1024 * 1024 - 65536
def params(**more):
    return pltpu.CompilerParams(vmem_limit_bytes=VMEM, **more)


def whole(shape):
    return pl.BlockSpec(shape, lambda *i: (0,) * len(shape), pipeline_mode=pl.Buffered(1))


def cost(flops, nbytes):
    return pl.CostEstimate(flops=flops, bytes_accessed=nbytes, transcendentals=0)


def place():
    s = lax.axis_index("s")
    return s // 2, s % 2, lax.axis_index("r")


def solution(mesh):
    ns, nr = mesh.shape["s"], mesh.shape["r"]
    nx = ns // 2
    assert nx == 4 and nr == 4

    def owner(x, c, xr, other):
        return 2 * ((x + xr) % nx) + (c + other) % 2

    def neighbours():
        s, y = lax.axis_index("s"), lax.axis_index("r")
        return s, y, {
            "core": {"s": s + 1 - 2 * (s % 2)},
            "right": {"s": (s + 2) % ns},
            "left": {"s": (s + ns - 2) % ns},
            "up": {"r": (y + 1) % nr},
            "below": {"r": (y + nr - 1) % nr},
            "pair": {"r": y + 1 - 2 * (y % 2)},
            "cross": {"r": nr - 1 - y},
        }

    def greet(to, names):
        barrier = pltpu.get_barrier_semaphore()
        for name in names:
            pl.semaphore_signal(barrier, inc=1, device_id=to[name], device_id_type=pl.DeviceIdType.MESH)
        pl.semaphore_wait(barrier, len(names))

    def remote(src, dst, send, recv, device):
        return pltpu.make_async_remote_copy(src_ref=src, dst_ref=dst, send_sem=send, recv_sem=recv, device_id=device, device_id_type=pl.DeviceIdType.MESH)

    class Summing:
        def __init__(self, mine, chunks):
            _, self.rows, self.n = mine.shape
            self.k, self.h = chunks, self.rows // chunks
            assert self.rows % chunks == 0 and self.h % 32 == 0
            self.last = chunks + 3
            whole_, halves, block = (nx, self.rows, self.n), (chunks, 2, self.h // 2, self.n), (chunks, self.h, self.n)
            self.in_specs = [pl.BlockSpec(memory_space=pl.ANY)] * 2
            self.out_spec = pl.BlockSpec((self.rows, self.n), lambda *i: (0, 0), pipeline_mode=pl.Buffered(1))
            self.out_shape = jax.ShapeDtypeStruct((self.rows, self.n), bf16)
            self.scratch = [pltpu.VMEM(s, bf16) for s in (whole_,) * 3 + (halves,) * 4 + (block,) * 4]
            self.scratch += [pltpu.SemaphoreType.DMA((chunks,)), pltpu.SemaphoreType.DMA((9, chunks)), pltpu.SemaphoreType.DMA((9, chunks))]

        def bind(self, mine, theirs, out, scratch):
            self.mine, self.theirs, self.out = mine, theirs, out
            self.own, self.other, self.t, self.far, self.near, self.acc, self.got, self.b1, self.y1, self.b2, self.y2, self.load_sem, self.send, self.recv = scratch
            _, _, self.to = neighbours()

        def part(self, k, half=None):
            if half is None:
                return pl.ds(pl.multiple_of(k * self.h, 32), self.h)
            return pl.ds(pl.multiple_of(k * self.h + half * (self.h // 2), 16), self.h // 2)

        def load(self, k):
            return pltpu.make_async_copy(self.mine.at[:, self.part(k)], self.own.at[:, self.part(k)], self.load_sem.at[k])

        def copy(self, which, k):
            src, dst, to = (
                lambda: (self.theirs.at[:, self.part(k)], self.other.at[:, self.part(k)], "core"),
                lambda: (self.t.at[2, self.part(k, 0)], self.far.at[k, 0], "left"),
                lambda: (self.t.at[2, self.part(k, 1)], self.far.at[k, 1], "right"),
                lambda: (self.t.at[1, self.part(k, 0)], self.near.at[k, 0], "right"),
                lambda: (self.t.at[3, self.part(k, 1)], self.near.at[k, 1], "left"),
                lambda: (self.acc.at[k, 0], self.got.at[k, 0], "left"),
                lambda: (self.acc.at[k, 1], self.got.at[k, 1], "right"),
                lambda: (self.b1.at[k], self.y1.at[k], "pair"),
                lambda: (self.b2.at[k], self.y2.at[k], "cross"),
            )[which]()
            return remote(src, dst, self.send.at[which, k], self.recv.at[which, k], self.to[to])

        def start(self):
            greet(self.to, ("core", "right", "left", "pair", "cross"))

            def go(k, _):
                self.copy(0, k).start()
                self.load(k).start()
                return 0

            lax.fori_loop(0, self.k, go, 0)

        def step(self, i):
            wide = lambda v: v.astype(f32)

            def when(k, f):
                if isinstance(k, int):
                    if 0 <= k < self.k:
                        f(k)
                else:
                    pl.when((k >= 0) & (k < self.k))(lambda: f(k))

            def cores(k):
                self.load(k).wait()
                self.copy(0, k).wait_recv()
                for p in (2, 1, 3, 0):
                    self.t[p, self.part(k)] = (wide(self.own[p, self.part(k)]) + wide(self.other[p, self.part(k)])).astype(bf16)
                for which in (1, 2, 3, 4):
                    self.copy(which, k).start()

            def far(k):
                for half, p in ((0, 3), (1, 1)):
                    self.copy(1 + half, k).wait_recv()
                    self.acc[k, half] = (wide(self.t[p, self.part(k, half)]) + wide(self.far[k, half])).astype(bf16)
                    self.copy(5 + half, k).start()

            def block(k):
                for half in (0, 1):
                    self.copy(3 + half, k).wait_recv()
                    self.copy(5 + half, k).wait_recv()
                    total = wide(self.t[0, self.part(k, half)]) + wide(self.near[k, half]) + wide(self.got[k, half])
                    self.b1[k, pl.ds(half * (self.h // 2), self.h // 2)] = total.astype(bf16)
                self.copy(7, k).start()

            def pair(k):
                self.copy(7, k).wait_recv()
                self.b2[k] = (wide(self.b1[k]) + wide(self.y1[k])).astype(bf16)
                self.copy(8, k).start()

            def cross(k):
                self.copy(8, k).wait_recv()
                self.out[self.part(k), :] = (wide(self.b2[k]) + wide(self.y2[k])).astype(bf16)

            for back, f in enumerate((cores, far, block, pair, cross)):
                when(i - back, f)

        def finish(self):
            def sent(k, _):
                for which in range(9):
                    self.copy(which, k).wait_send()
                return 0

            lax.fori_loop(0, self.k, sent, 0)

    def fetched(gate, up):
        rows, ff = gate.shape
        n = rows // nr
        count = 48

        def kernel(g_ref, u_ref, out, buf, local, send, recv):
            s, y, to = neighbours()
            o = {"L": (s + ns - 2) % ns, "R": (s + 2) % ns, "F": (s + ns // 2) % ns}
            q = {0: y, -1: (y + nr - 1) % nr, 1: (y + 1) % nr, 2: (y + 2) % nr}
            used = []

            def put(src, dst, name):
                i = len(used)
                c = remote(src, dst, send.at[i], recv.at[i], to[name])
                c.start()
                used.append(c)
                return c

            def pass_on(ref, name):
                return put(ref, ref, name)

            greet(to, ("core", "right", "left", "up", "below"))
            loads = [pltpu.make_async_copy(r, buf.at[m], local.at[m]) for m, r in enumerate((g_ref, u_ref))]
            for c in loads:
                c.start()
            mine = pl.multiple_of(y * n, 16)

            def rows_of(who, share, half=None):
                first, many = (0, n) if half is None else (half * (n // 2), n // 2)
                return out.at[o[who], 1, pl.ds(pl.multiple_of(q[share] * n + first, 16), many)]

            src = u_ref.at[pl.ds(mine, n)]
            dst = out.at[s, 1, pl.ds(mine, n)]
            from_left, from_right = put(src, dst, "right"), put(src, dst, "left")
            a_left, a_right = put(g_ref, out.at[s, 0], "right"), put(g_ref, out.at[s, 0], "left")
            cores = [put(g_ref, out.at[s, 0], "core"), put(u_ref, out.at[s, 1], "core")]
            up_from, below_from = {}, {}
            late = []
            for c, who, half in ((from_left, "L", None), (from_right, "R", None), (None, "F", 0), (None, "F", 1)):
                if half is not None:
                    c = fars[half]
                c.wait_recv()
                if who == "L":
                    fars = [pass_on(rows_of("L", 0, 0), "right"), None]
                elif who == "R":
                    fars[1] = pass_on(rows_of("R", 0, 1), "left")
                ref = rows_of(who, 0, half)
                below_from[who, half] = pass_on(ref, "up")
                up_from[who, half] = pass_on(ref, "below")
                cores.append(pass_on(ref, "core"))
            half = rows // 2
            a_left.wait_recv()
            far_upper = pass_on(out.at[o["L"], 0, pl.ds(0, half)], "right")
            cores.append(pass_on(out.at[o["L"], 0], "core"))
            a_right.wait_recv()
            far_lower = pass_on(out.at[o["R"], 0, pl.ds(half, half)], "left")
            cores.append(pass_on(out.at[o["R"], 0], "core"))
            for c in loads:
                c.wait()
            store = pltpu.make_async_copy(buf, out.at[s], local.at[2])
            store.start()
            for who, part in (("L", None), ("R", None), ("F", 0), ("F", 1)):
                below_from[who, part].wait_recv()
                ref = rows_of(who, -1, part)
                if (who, part) in (("L", None), ("F", 0)):
                    late.append((pass_on(ref, "up"), rows_of(who, 2, part)))
                cores.append(pass_on(ref, "core"))
                up_from[who, part].wait_recv()
                ref = rows_of(who, 1, part)
                if (who, part) in (("R", None), ("F", 1)):
                    late.append((pass_on(ref, "below"), rows_of(who, 2, part)))
                cores.append(pass_on(ref, "core"))
            for c, ref in late:
                c.wait_recv()
                cores.append(pass_on(ref, "core"))
            far_upper.wait_recv()
            cores.append(pass_on(out.at[o["F"], 0, pl.ds(0, half)], "core"))
            far_lower.wait_recv()
            cores.append(pass_on(out.at[o["F"], 0, pl.ds(half, half)], "core"))
            for c in cores:
                c.wait_recv()
            for c in used:
                c.wait_send()
            store.wait()
            assert len(used) <= count

        anywhere = pl.BlockSpec(memory_space=pl.ANY)
        return pl.pallas_call(
            kernel,
            name="fetched",
            in_specs=[anywhere] * 2,
            out_specs=anywhere,
            out_shape=jax.ShapeDtypeStruct((ns, 2, rows, ff), bf16),
            scratch_shapes=[pltpu.VMEM((2, rows, ff), bf16), pltpu.SemaphoreType.DMA((3,)), pltpu.SemaphoreType.DMA((count,)), pltpu.SemaphoreType.DMA((count,))],
            compiler_params=params(collective_id=0, has_side_effects=True),
            cost_estimate=cost(20 * 1000 * 1000 * 1000, 4 * ns * rows * ff),
        )(gate, up)

    def gate_up(h, pair):
        t, d = h.shape
        ff = pair.shape[-1]
        r = 512
        steps = t // r
        share = d // ns
        groups = [(0, WIDE), (WIDE, ff)]

        def kernel(h_ref, pair_ref, s1, s2, act_o, actt_o, at_o, w_s, a_s, sem):
            i = pl.program_id(0)

            def load(m, k):
                lo, hi = groups[k]
                return pltpu.make_async_copy(pair_ref.at[:, m, :, pl.ds(lo, hi - lo)], w_s.at[m, :, :, pl.ds(lo, hi - lo)], sem.at[m, k])

            @pl.when(i == 0)
            def _():
                for k in range(len(groups)):
                    for m in range(2):
                        load(m, k).start()

            w = h_ref[...].astype(f32)
            a_s[...] = (w * lax.rsqrt(jnp.mean(w * w, -1, keepdims=True) + EPS)).astype(bf16)
            x, c, _ = place()
            for p in range(ns):
                s = owner(x, c, p % nx, p // nx)
                at_o[p * share : (p + 1) * share, :] = a_s[:, pl.ds(pl.multiple_of(s * share, share), share)].T
            for k in range(0, ff, WIDE):
                if k <= WIDE:
                    @pl.when(i == 0)
                    def _(k=k):
                        for m in range(2):
                            load(m, k // WIDE).wait()
                cols = slice(k, k + WIDE)
                a = a_s[...]
                g, u = (jnp.dot(a, w_s[m, :, :, cols].reshape(d, WIDE), preferred_element_type=f32) for m in range(2))
                sg = jax.nn.sigmoid(g)
                silu = g * sg
                s1[:, cols] = silu
                s2[:, cols] = u * (sg + silu * (1 - sg))
                act = (silu * u).astype(bf16)
                act_o[:, cols] = act
                actt_o[cols, :] = act.T

        rows = lambda n: pl.BlockSpec((r, n), lambda i: (i, 0))
        cols = lambda n: pl.BlockSpec((n, r), lambda i: (0, i))
        shape = jax.ShapeDtypeStruct
        return pl.pallas_call(
            kernel,
            grid=(steps,),
            name="gate_up",
            in_specs=[rows(d), pl.BlockSpec(memory_space=pl.ANY)],
            out_specs=[rows(ff), rows(ff), rows(ff), cols(ff), cols(d)],
            out_shape=[shape((t, ff), f32), shape((t, ff), f32), shape((t, ff), bf16), shape((ff, t), bf16), shape((d, t), bf16)],
            scratch_shapes=[pltpu.VMEM((2, ns, share, ff), bf16), pltpu.VMEM((r, d), bf16), pltpu.SemaphoreType.DMA((2, 2))],
            compiler_params=params(),
            cost_estimate=cost(4 * t * d * ff, 14 * t * ff),
        )(h, pair)

    def down(h, act, w):
        t, d = h.shape
        ff = act.shape[1]
        r = 512

        def kernel(h_ref, act_ref, w_ref, o_ref):
            y = jnp.dot(act_ref[...], w_ref[...], preferred_element_type=f32).astype(bf16)
            o_ref[...] = (h_ref[...].astype(f32) + y.astype(f32)).astype(bf16)

        rows = lambda n: pl.BlockSpec((r, n), lambda i: (i, 0))
        return pl.pallas_call(
            kernel,
            grid=(t // r,),
            name="down",
            in_specs=[rows(d), rows(ff), whole((ff, d))],
            out_specs=rows(d),
            out_shape=jax.ShapeDtypeStruct((t, d), bf16),
            compiler_params=params(),
            cost_estimate=cost(2 * t * d * ff, 2 * t * ff),
        )(h, act, w)

    def by_down(actt, dy, split):
        ff, t = actt.shape
        d = dy.shape[1]
        pair = ff // nx
        share = pair // 2

        def kernel(pos, actt_ref, dy_ref, *out):
            w = jnp.dot(actt_ref[...], dy_ref[...], preferred_element_type=f32).astype(bf16)
            if not split:
                out[0][...] = w
                return
            mine, theirs = out
            c = lax.axis_index("s") % 2

            @pl.when(c == 0)
            def _():
                mine[0], theirs[0] = w[:share], w[share:]

            @pl.when(c == 1)
            def _():
                mine[0], theirs[0] = w[share:], w[:share]

        block = pl.BlockSpec((1, share, d), lambda i, pos: (i, 0, 0))
        first = (lax.axis_index("s") // 2 if split else jnp.int32(0)).astype(jnp.int32)
        return pl.pallas_call(
            kernel,
            name="by_down",
            grid_spec=pltpu.PrefetchScalarGridSpec(
                num_scalar_prefetch=1,
                grid=(nx,),
                in_specs=[pl.BlockSpec((pair, t), lambda i, pos: ((pos[0] + i) % nx, 0)), pl.BlockSpec((t, d), lambda i, pos: (0, 0), pipeline_mode=pl.Buffered(1))],
                out_specs=[block, block] if split else pl.BlockSpec((pair, d), lambda i, pos: (i, 0)),
            ),
            out_shape=[jax.ShapeDtypeStruct((nx, share, d), bf16)] * 2 if split else jax.ShapeDtypeStruct((ff, d), bf16),
            compiler_params=params(),
            cost_estimate=cost(2 * t * d * ff, 2 * t * ff),
        )(first[None], actt, dy)

    def by_gate_up(dy, at, w, s1, s2, terms=None):
        t, d = dy.shape
        share = d // ns
        ff = s1.shape[1]
        r = 512
        work = Summing(terms[0], 5) if terms else None

        def kernel(*refs):
            if work:
                dy_ref, at_hbm, w_ref, s1_ref, s2_ref, m_ref, t_ref, dg, du, mine, theirs, out, at_ref, sem, *scratch = refs
                work.bind(m_ref, t_ref, out, scratch)
            else:
                dy_ref, at_hbm, w_ref, s1_ref, s2_ref, dg, du, plain, at_ref, sem = refs
            x, c, _ = place()
            load = pltpu.make_async_copy(at_hbm, at_ref, sem)
            j = pl.program_id(0)

            @pl.when(j == 0)
            def _():
                load.start()
                if work:
                    work.start()

            for k in range(0, t, r):
                rows = slice(k, k + r)
                back = lax.dot_general(dy_ref[rows, :], w_ref[...], NT, preferred_element_type=f32).astype(bf16).astype(f32)
                dg[rows, :] = (back * s2_ref[rows, :]).astype(bf16)
                du[rows, :] = (back * s1_ref[rows, :]).astype(bf16)

            @pl.when(j == 0)
            def _():
                load.wait()

            for k, ref in enumerate((dg, du)):
                if work:
                    work.step(2 * j + k)
                term = jnp.dot(at_ref[...], ref[...], preferred_element_type=f32).astype(bf16)
                to = slice(k * share, (k + 1) * share)
                for p in range(ns):
                    block = term[p * share : (p + 1) * share]
                    if not work:
                        plain[owner(x, c, p % nx, p // nx), to] = block
                    elif p < nx:
                        mine[p, to] = block
                    else:
                        theirs[p - nx, to] = block

            if work:
                assert work.last < 2 * (ff // WIDE)

                @pl.when(j == ff // WIDE - 1)
                def _():
                    work.finish()

        cols = lambda n: pl.BlockSpec((n, WIDE), lambda j: (0, j))
        many, parts = (2, nx) if work else (1, ns)
        block = pl.BlockSpec((parts, 2 * share, WIDE), lambda j: (0, 0, j))
        shape = jax.ShapeDtypeStruct
        return pl.pallas_call(
            kernel,
            grid=(ff // WIDE,),
            name="by_gate_up",
            in_specs=[whole((t, d)), pl.BlockSpec(memory_space=pl.ANY), pl.BlockSpec((WIDE, d), lambda j: (j, 0)), cols(t), cols(t)] + (work.in_specs if work else []),
            out_specs=[cols(t), cols(t)] + [block] * many + ([work.out_spec] if work else []),
            out_shape=[shape((t, ff), bf16)] * 2 + [shape((parts, 2 * share, ff), bf16)] * many + ([work.out_shape] if work else []),
            scratch_shapes=[pltpu.VMEM((d, t), bf16), pltpu.SemaphoreType.DMA(())] + (work.scratch if work else []),
            compiler_params=params(collective_id=1, has_side_effects=True) if work else params(),
            cost_estimate=cost(6 * t * d * ff, 12 * t * ff),
        )(dy, at, w, s1, s2, *(terms or ()))

    def by_input(dg, du, pair, h, dy, terms=None):
        t, d = h.shape
        ff = dg.shape[1]
        share = d // ns
        r = 256
        steps = t // r
        work = Summing(terms[0], 8) if terms else None

        def kernel(*refs):
            if work:
                dg_ref, du_ref, wg_ref, wu_ref, h_ref, dy_ref, m_ref, t_ref, o_ref, out, *scratch = refs
                work.bind(m_ref, t_ref, out, scratch)

                @pl.when(pl.program_id(0) == 0)
                def _():
                    work.start()
            else:
                dg_ref, du_ref, wg_ref, wu_ref, h_ref, dy_ref, o_ref = refs
            da = sum(
                lax.dot_general(x[...], w[...].reshape(d, ff), NT, preferred_element_type=f32) for x, w in ((dg_ref, wg_ref), (du_ref, wu_ref))
            )
            wide = h_ref[...].astype(f32)
            scale = lax.rsqrt(jnp.mean(wide * wide, -1, keepdims=True) + EPS)
            back = scale * (da - wide * (scale * scale * jnp.mean(da * wide, -1, keepdims=True)))
            o_ref[...] = (dy_ref[...].astype(f32) + back).astype(bf16)
            if work:
                work.step(pl.program_id(0))

                @pl.when(pl.program_id(0) == steps - 1)
                def _():
                    def rest(i, _):
                        work.step(i)
                        return 0

                    lax.fori_loop(steps, work.last + 1, rest, 0)
                    work.finish()

        rows = lambda n: pl.BlockSpec((r, n), lambda i: (i, 0))
        matrix = lambda m: pl.BlockSpec((ns, None, share, ff), lambda i: (0, m, 0, 0), pipeline_mode=pl.Buffered(1))
        shape = jax.ShapeDtypeStruct((t, d), bf16)
        return pl.pallas_call(
            kernel,
            grid=(steps,),
            name="by_input",
            in_specs=[rows(ff)] * 2 + [matrix(0), matrix(1)] + [rows(d)] * 2 + (work.in_specs if work else []),
            out_specs=[rows(d), work.out_spec] if work else rows(d),
            out_shape=[shape, work.out_shape] if work else shape,
            scratch_shapes=work.scratch if work else [],
            compiler_params=params(collective_id=2, has_side_effects=True) if work else params(),
            cost_estimate=cost(4 * t * d * ff, 4 * t * ff),
        )(dg, du, pair, pair, h, dy, *(terms or ()))

    def step(x, dy, *weights):
        layers, share, _ = weights[0].shape
        h, dy = x[0], dy[0]
        summed = lambda term: lax.psum(lax.psum_scatter(term, "s", scatter_dimension=0, tiled=True), "r")
        whole_of = lambda w: lax.all_gather(w, "s", axis=0, tiled=True)

        kept = []
        for number in range(layers):
            gate, up = weights[0][number], weights[1][number]
            if number == 0:
                pair = fetched(gate, up)
            else:
                pair = whole_of(jnp.concatenate([gate, up])).reshape(ns, 2, share, -1)
            wd = whole_of(weights[2][number])
            s1, s2, act, actt, at = gate_up(h, pair)
            kept.append((h, s1, s2, actt, at, pair, wd))
            if number < layers - 1:
                h = down(h, act, wd)
        grads = [None] * layers
        for number in reversed(range(layers)):
            h, s1, s2, actt, at, pair, wd = kept[number]
            down_terms = by_down(actt, dy, number == 0)
            if number == 0:
                dg, du, *terms, g_down = by_gate_up(dy, at, wd, s1, s2, down_terms)
                dy, g_pair = by_input(dg, du, pair, h, dy, terms)
            else:
                dg, du, terms = by_gate_up(dy, at, wd, s1, s2)
                dy = by_input(dg, du, pair, h, dy)
                g_down, g_pair = (summed(v) for v in (down_terms, terms.reshape(2 * share * ns, -1)))
            grads[number] = (g_pair[:share], g_pair[share:], g_down)
        return (dy[None], *(jnp.stack([g[i] for g in grads]) for i in range(3)))

    states, cut = P(("rep", "r", "s"), None, None), P(None, "s", None)
    return jax.shard_map(
        step,
        mesh=mesh,
        in_specs=(states, states) + (cut,) * 3,
        out_specs=(states,) + (P("rep", "s", None),) * 3,
        check_vma=False,
    )
```

```python
import jax
import jax.numpy as jnp
from jax import lax
from jax.experimental import pallas as pl
from jax.experimental.pallas import tpu as pltpu
from jax.sharding import PartitionSpec as P

bf16, f32 = jnp.bfloat16, jnp.float32
NT = (((1,), (1,)), ((), ()))
EPS = 1e-6
WIDE = 512
FIRST = 3
VMEM = 64 * 1024 * 1024 - 65536


def params(**more):
    return pltpu.CompilerParams(vmem_limit_bytes=VMEM, **more)


def whole(shape):
    return pl.BlockSpec(shape, lambda *i: (0,) * len(shape), pipeline_mode=pl.Buffered(1))


def cost(flops, nbytes):
    return pl.CostEstimate(flops=flops, bytes_accessed=nbytes, transcendentals=0)


def place():
    s = lax.axis_index("s")
    return s // 2, s % 2, lax.axis_index("r")


def solution(mesh):
    ns, nr = mesh.shape["s"], mesh.shape["r"]
    nx = ns // 2
    assert nx == 4 and nr == 4

    def owner(x, c, xr, other):
        return 2 * ((x + xr) % nx) + (c + other) % 2

    def neighbours():
        s, y = lax.axis_index("s"), lax.axis_index("r")
        return s, y, {
            "core": {"s": s + 1 - 2 * (s % 2)},
            "right": {"s": (s + 2) % ns},
            "left": {"s": (s + ns - 2) % ns},
            "up": {"r": (y + 1) % nr},
            "below": {"r": (y + nr - 1) % nr},
            "pair": {"r": y + 1 - 2 * (y % 2)},
            "cross": {"r": nr - 1 - y},
        }

    def greet(to, names):
        barrier = pltpu.get_barrier_semaphore()
        for name in names:
            pl.semaphore_signal(barrier, inc=1, device_id=to[name], device_id_type=pl.DeviceIdType.MESH)
        pl.semaphore_wait(barrier, len(names))

    def remote(src, dst, send, recv, device):
        return pltpu.make_async_remote_copy(src_ref=src, dst_ref=dst, send_sem=send, recv_sem=recv, device_id=device, device_id_type=pl.DeviceIdType.MESH)

    class Summing:
        def __init__(self, mine, chunks):
            _, self.rows, self.n = mine.shape
            self.k, self.h = chunks, self.rows // chunks
            assert self.rows % chunks == 0 and self.h % 32 == 0
            self.last = chunks + 3
            whole_, halves, block = (nx, self.rows, self.n), (chunks, 2, self.h // 2, self.n), (chunks, self.h, self.n)
            self.in_specs = [pl.BlockSpec(memory_space=pl.ANY)] * 2
            self.out_spec = pl.BlockSpec((self.rows, self.n), lambda *i: (0, 0), pipeline_mode=pl.Buffered(1))
            self.out_shape = jax.ShapeDtypeStruct((self.rows, self.n), bf16)
            self.scratch = [pltpu.VMEM(s, bf16) for s in (whole_,) * 3 + (halves,) * 4 + (block,) * 4]
            self.scratch += [pltpu.SemaphoreType.DMA((chunks,)), pltpu.SemaphoreType.DMA((9, chunks)), pltpu.SemaphoreType.DMA((9, chunks))]

        def bind(self, mine, theirs, out, scratch):
            self.mine, self.theirs, self.out = mine, theirs, out
            self.own, self.other, self.t, self.far, self.near, self.acc, self.got, self.b1, self.y1, self.b2, self.y2, self.load_sem, self.send, self.recv = scratch
            _, _, self.to = neighbours()

        def part(self, k, half=None):
            if half is None:
                return pl.ds(pl.multiple_of(k * self.h, 32), self.h)
            return pl.ds(pl.multiple_of(k * self.h + half * (self.h // 2), 16), self.h // 2)

        def load(self, k):
            return pltpu.make_async_copy(self.mine.at[:, self.part(k)], self.own.at[:, self.part(k)], self.load_sem.at[k])

        def copy(self, which, k):
            src, dst, to = (
                lambda: (self.theirs.at[:, self.part(k)], self.other.at[:, self.part(k)], "core"),
                lambda: (self.t.at[2, self.part(k, 0)], self.far.at[k, 0], "left"),
                lambda: (self.t.at[2, self.part(k, 1)], self.far.at[k, 1], "right"),
                lambda: (self.t.at[1, self.part(k, 0)], self.near.at[k, 0], "right"),
                lambda: (self.t.at[3, self.part(k, 1)], self.near.at[k, 1], "left"),
                lambda: (self.acc.at[k, 0], self.got.at[k, 0], "left"),
                lambda: (self.acc.at[k, 1], self.got.at[k, 1], "right"),
                lambda: (self.b1.at[k], self.y1.at[k], "pair"),
                lambda: (self.b2.at[k], self.y2.at[k], "cross"),
            )[which]()
            return remote(src, dst, self.send.at[which, k], self.recv.at[which, k], self.to[to])

        def start(self):
            greet(self.to, ("core", "right", "left", "pair", "cross"))

            def go(k, _):
                self.copy(0, k).start()
                self.load(k).start()
                return 0

            lax.fori_loop(0, self.k, go, 0)

        def step(self, i):
            wide = lambda v: v.astype(f32)

            def when(k, f):
                if isinstance(k, int):
                    if 0 <= k < self.k:
                        f(k)
                else:
                    pl.when((k >= 0) & (k < self.k))(lambda: f(k))

            def cores(k):
                self.load(k).wait()
                self.copy(0, k).wait_recv()
                for p in (2, 1, 3, 0):
                    self.t[p, self.part(k)] = (wide(self.own[p, self.part(k)]) + wide(self.other[p, self.part(k)])).astype(bf16)
                for which in (1, 2, 3, 4):
                    self.copy(which, k).start()

            def far(k):
                for half, p in ((0, 3), (1, 1)):
                    self.copy(1 + half, k).wait_recv()
                    self.acc[k, half] = (wide(self.t[p, self.part(k, half)]) + wide(self.far[k, half])).astype(bf16)
                    self.copy(5 + half, k).start()

            def block(k):
                for half in (0, 1):
                    self.copy(3 + half, k).wait_recv()
                    self.copy(5 + half, k).wait_recv()
                    total = wide(self.t[0, self.part(k, half)]) + wide(self.near[k, half]) + wide(self.got[k, half])
                    self.b1[k, pl.ds(half * (self.h // 2), self.h // 2)] = total.astype(bf16)
                self.copy(7, k).start()

            def pair(k):
                self.copy(7, k).wait_recv()
                self.b2[k] = (wide(self.b1[k]) + wide(self.y1[k])).astype(bf16)
                self.copy(8, k).start()

            def cross(k):
                self.copy(8, k).wait_recv()
                self.out[self.part(k), :] = (wide(self.b2[k]) + wide(self.y2[k])).astype(bf16)

            for back, f in enumerate((cores, far, block, pair, cross)):
                when(i - back, f)

        def finish(self):
            def sent(k, _):
                for which in range(9):
                    self.copy(which, k).wait_send()
                return 0

            lax.fori_loop(0, self.k, sent, 0)

    def fetched(gate, up):
        rows, ff = gate.shape
        n = rows // nr
        count = 80

        def kernel(g_ref, u_ref, out, buf, local, send, recv):
            s, y, to = neighbours()
            o = {"L": (s + ns - 2) % ns, "R": (s + 2) % ns, "F": (s + ns // 2) % ns}
            q = {0: y, -1: (y + nr - 1) % nr, 1: (y + 1) % nr, 2: (y + 2) % nr}
            used = []

            def put(src, dst, name):
                i = len(used)
                c = remote(src, dst, send.at[i], recv.at[i], to[name])
                c.start()
                used.append(c)
                return c

            def pass_on(ref, name):
                return put(ref, ref, name)

            greet(to, ("core", "right", "left", "up", "below"))
            loads = [pltpu.make_async_copy(r, buf.at[m], local.at[m]) for m, r in enumerate((g_ref, u_ref))]
            for c in loads:
                c.start()
            mine = pl.multiple_of(y * n, 16)

            def rows_of(m, who, share, half=None):
                first, many = (0, n) if half is None else (half * (n // 2), n // 2)
                return out.at[o[who], m, pl.ds(pl.multiple_of(q[share] * n + first, 16), many)]

            firsts = {}
            for m, ref in enumerate((g_ref, u_ref)):
                src, dst = ref.at[pl.ds(mine, n)], out.at[s, m, pl.ds(mine, n)]
                firsts[m, "L"], firsts[m, "R"] = put(src, dst, "right"), put(src, dst, "left")
            cores = [put(ref, out.at[s, m], "core") for m, ref in enumerate((g_ref, u_ref))]
            up_from, below_from, late = {}, {}, []
            for m in range(2):
                for who, half in (("L", None), ("R", None), ("F", 0), ("F", 1)):
                    firsts[(m, who) if half is None else (m, who, half)].wait_recv()
                    if who == "L":
                        firsts[m, "F", 0] = pass_on(rows_of(m, "L", 0, 0), "right")
                    elif who == "R":
                        firsts[m, "F", 1] = pass_on(rows_of(m, "R", 0, 1), "left")
                    ref = rows_of(m, who, 0, half)
                    below_from[m, who, half] = pass_on(ref, "up")
                    up_from[m, who, half] = pass_on(ref, "below")
                    cores.append(pass_on(ref, "core"))
            for c in loads:
                c.wait()
            store = pltpu.make_async_copy(buf, out.at[s], local.at[2])
            store.start()
            for m in range(2):
                for who, part in (("L", None), ("R", None), ("F", 0), ("F", 1)):
                    below_from[m, who, part].wait_recv()
                    ref = rows_of(m, who, -1, part)
                    if (who, part) in (("L", None), ("F", 0)):
                        late.append((pass_on(ref, "up"), rows_of(m, who, 2, part)))
                    cores.append(pass_on(ref, "core"))
                    up_from[m, who, part].wait_recv()
                    ref = rows_of(m, who, 1, part)
                    if (who, part) in (("R", None), ("F", 1)):
                        late.append((pass_on(ref, "below"), rows_of(m, who, 2, part)))
                    cores.append(pass_on(ref, "core"))
            for c, ref in late:
                c.wait_recv()
                cores.append(pass_on(ref, "core"))
            for c in cores:
                c.wait_recv()
            for c in used:
                c.wait_send()
            store.wait()
            assert len(used) <= count

        anywhere = pl.BlockSpec(memory_space=pl.ANY)
        return pl.pallas_call(
            kernel,
            name="fetched",
            in_specs=[anywhere] * 2,
            out_specs=anywhere,
            out_shape=jax.ShapeDtypeStruct((ns, 2, rows, ff), bf16),
            scratch_shapes=[pltpu.VMEM((2, rows, ff), bf16), pltpu.SemaphoreType.DMA((3,)), pltpu.SemaphoreType.DMA((count,)), pltpu.SemaphoreType.DMA((count,))],
            compiler_params=params(collective_id=0, has_side_effects=True),
            cost_estimate=cost(20 * 1000 * 1000 * 1000, 4 * ns * rows * ff),
        )(gate, up)

    def gate_up(h, pair):
        t, d = h.shape
        ff = pair.shape[-1]
        r = 512
        steps = t // r
        share = d // ns
        groups = [(0, WIDE), (WIDE, ff)]

        def kernel(h_ref, pair_ref, s1, s2, act_o, actt_o, at_o, w_s, a_s, sem):
            i = pl.program_id(0)

            def load(m, k):
                lo, hi = groups[k]
                return pltpu.make_async_copy(pair_ref.at[:, m, :, pl.ds(lo, hi - lo)], w_s.at[m, :, :, pl.ds(lo, hi - lo)], sem.at[m, k])

            @pl.when(i == 0)
            def _():
                for k in range(len(groups)):
                    for m in range(2):
                        load(m, k).start()

            w = h_ref[...].astype(f32)
            a_s[...] = (w * lax.rsqrt(jnp.mean(w * w, -1, keepdims=True) + EPS)).astype(bf16)
            x, c, _ = place()
            for p in range(ns):
                s = owner(x, c, p % nx, p // nx)
                at_o[p * share : (p + 1) * share, :] = a_s[:, pl.ds(pl.multiple_of(s * share, share), share)].T
            for k in range(0, ff, WIDE):
                if k <= WIDE:
                    @pl.when(i == 0)
                    def _(k=k):
                        for m in range(2):
                            load(m, k // WIDE).wait()
                cols = slice(k, k + WIDE)
                a = a_s[...]
                g, u = (jnp.dot(a, w_s[m, :, :, cols].reshape(d, WIDE), preferred_element_type=f32) for m in range(2))
                sg = jax.nn.sigmoid(g)
                silu = g * sg
                s1[:, cols] = silu
                s2[:, cols] = u * (sg + silu * (1 - sg))
                act = (silu * u).astype(bf16)
                act_o[:, cols] = act
                actt_o[cols, :] = act.T

        rows = lambda n: pl.BlockSpec((r, n), lambda i: (i, 0))
        cols = lambda n: pl.BlockSpec((n, r), lambda i: (0, i))
        shape = jax.ShapeDtypeStruct
        return pl.pallas_call(
            kernel,
            grid=(steps,),
            name="gate_up",
            in_specs=[rows(d), pl.BlockSpec(memory_space=pl.ANY)],
            out_specs=[rows(ff), rows(ff), rows(ff), cols(ff), cols(d)],
            out_shape=[shape((t, ff), f32), shape((t, ff), f32), shape((t, ff), bf16), shape((ff, t), bf16), shape((d, t), bf16)],
            scratch_shapes=[pltpu.VMEM((2, ns, share, ff), bf16), pltpu.VMEM((r, d), bf16), pltpu.SemaphoreType.DMA((2, 2))],
            compiler_params=params(),
            cost_estimate=cost(4 * t * d * ff, 14 * t * ff),
        )(h, pair)

    def down(h, act, w):
        t, d = h.shape
        ff = act.shape[1]
        r = 512

        def kernel(h_ref, act_ref, w_ref, o_ref):
            y = jnp.dot(act_ref[...], w_ref[...], preferred_element_type=f32).astype(bf16)
            o_ref[...] = (h_ref[...].astype(f32) + y.astype(f32)).astype(bf16)

        rows = lambda n: pl.BlockSpec((r, n), lambda i: (i, 0))
        return pl.pallas_call(
            kernel,
            grid=(t // r,),
            name="down",
            in_specs=[rows(d), rows(ff), whole((ff, d))],
            out_specs=rows(d),
            out_shape=jax.ShapeDtypeStruct((t, d), bf16),
            compiler_params=params(),
            cost_estimate=cost(2 * t * d * ff, 2 * t * ff),
        )(h, act, w)

    def by_down(actt, dy, split):
        ff, t = actt.shape
        d = dy.shape[1]
        pair = ff // nx
        share = pair // 2

        def kernel(pos, actt_ref, dy_ref, *out):
            w = jnp.dot(actt_ref[...], dy_ref[...], preferred_element_type=f32).astype(bf16)
            if not split:
                out[0][...] = w
                return
            mine, theirs = out
            c = lax.axis_index("s") % 2

            @pl.when(c == 0)
            def _():
                mine[0], theirs[0] = w[:share], w[share:]

            @pl.when(c == 1)
            def _():
                mine[0], theirs[0] = w[share:], w[:share]

        block = pl.BlockSpec((1, share, d), lambda i, pos: (i, 0, 0))
        first = (lax.axis_index("s") // 2 if split else jnp.int32(0)).astype(jnp.int32)
        return pl.pallas_call(
            kernel,
            name="by_down",
            grid_spec=pltpu.PrefetchScalarGridSpec(
                num_scalar_prefetch=1,
                grid=(nx,),
                in_specs=[pl.BlockSpec((pair, t), lambda i, pos: ((pos[0] + i) % nx, 0)), pl.BlockSpec((t, d), lambda i, pos: (0, 0), pipeline_mode=pl.Buffered(1))],
                out_specs=[block, block] if split else pl.BlockSpec((pair, d), lambda i, pos: (i, 0)),
            ),
            out_shape=[jax.ShapeDtypeStruct((nx, share, d), bf16)] * 2 if split else jax.ShapeDtypeStruct((ff, d), bf16),
            compiler_params=params(),
            cost_estimate=cost(2 * t * d * ff, 2 * t * ff),
        )(first[None], actt, dy)

    def by_gate_up(dy, at, w, s1, s2, first, blocks, terms=None, chunks=None, slots=None, number=None):
        t, d = dy.shape
        share = d // ns
        ff = blocks * WIDE
        r = 512
        work = Summing(terms[0], chunks) if terms else None

        def kernel(*refs):
            if work:
                dy_ref, at_hbm, w_ref, s1_ref, s2_ref, m_ref, t_ref, dg, du, mine, theirs, out, at_ref, sem, *scratch = refs
                work.bind(m_ref, t_ref, out, scratch)
            else:
                dy_ref, at_hbm, w_ref, s1_ref, s2_ref, dg, du, plain, at_ref, sem = refs
            x, c, _ = place()
            load = pltpu.make_async_copy(at_hbm, at_ref, sem)
            j = pl.program_id(0)

            @pl.when(j == 0)
            def _():
                load.start()
                if work:
                    work.start()

            def turn(at_slot):
                if work and at_slot in slots:
                    work.step(len(slots) * j + slots.index(at_slot))

            for k in range(0, t, r):
                rows = slice(k, k + r)
                back = lax.dot_general(dy_ref[rows, :], w_ref[...], NT, preferred_element_type=f32).astype(bf16).astype(f32)
                dg[rows, :] = (back * s2_ref[rows, :]).astype(bf16)
                du[rows, :] = (back * s1_ref[rows, :]).astype(bf16)
                turn(k // r)

            @pl.when(j == 0)
            def _():
                load.wait()

            for k, ref in enumerate((dg, du)):
                term = jnp.dot(at_ref[...], ref[...], preferred_element_type=f32).astype(bf16)
                to = slice(k * share, (k + 1) * share)
                for p in range(ns):
                    block = term[p * share : (p + 1) * share]
                    if not work:
                        plain[owner(x, c, p % nx, p // nx), to] = block
                    elif p < nx:
                        mine[p, to] = block
                    else:
                        theirs[p - nx, to] = block
                turn(t // r + k)

            if work:
                @pl.when(j == blocks - 1)
                def _():
                    def rest(i, _):
                        work.step(i)
                        return 0

                    lax.fori_loop(blocks * len(slots), work.last + 1, rest, 0)
                    work.finish()

        cols = lambda n: pl.BlockSpec((n, WIDE), lambda j: (0, first + j))
        own = lambda n: pl.BlockSpec((n, WIDE), lambda j: (0, j))
        many, parts = (2, nx) if work else (1, ns)
        block = pl.BlockSpec((parts, 2 * share, WIDE), lambda j: (0, 0, j))
        shape = jax.ShapeDtypeStruct
        return pl.pallas_call(
            kernel,
            grid=(blocks,),
            name="by_gate_up",
            in_specs=[whole((t, d)), pl.BlockSpec(memory_space=pl.ANY), pl.BlockSpec((WIDE, d), lambda j: (first + j, 0)), cols(t), cols(t)] + (work.in_specs if work else []),
            out_specs=[own(t), own(t)] + [block] * many + ([work.out_spec] if work else []),
            out_shape=[shape((t, ff), bf16)] * 2 + [shape((parts, 2 * share, ff), bf16)] * many + ([work.out_shape] if work else []),
            scratch_shapes=[pltpu.VMEM((d, t), bf16), pltpu.SemaphoreType.DMA(())] + (work.scratch if work else []),
            compiler_params=params(collective_id=number, has_side_effects=True) if work else params(),
            cost_estimate=cost(6 * t * d * ff, 12 * t * ff),
        )(dy, at, w, s1, s2, *(terms or ()))

    def by_input(dgs, dus, pair, h, dy, terms=None):
        t, d = h.shape
        ff = pair.shape[-1]
        share = d // ns
        many = len(dgs)
        r = 256
        steps = t // r
        work = Summing(terms[0], 8) if terms else None

        def kernel(*refs):
            dg_refs, du_refs, refs = refs[:many], refs[many : 2 * many], refs[2 * many :]
            if work:
                wg_ref, wu_ref, h_ref, dy_ref, m_ref, t_ref, o_ref, out, *scratch = refs
                work.bind(m_ref, t_ref, out, scratch)

                @pl.when(pl.program_id(0) == 0)
                def _():
                    work.start()
            else:
                wg_ref, wu_ref, h_ref, dy_ref, o_ref = refs
            da, k = 0, 0
            for dg_ref, du_ref in zip(dg_refs, du_refs, strict=True):
                n = dg_ref.shape[1]
                for x, w in ((dg_ref, wg_ref), (du_ref, wu_ref)):
                    da += lax.dot_general(x[...], w[:, :, k : k + n].reshape(d, n), NT, preferred_element_type=f32)
                if work and k == 0:
                    work.step(2 * pl.program_id(0))
                k += n
            wide = h_ref[...].astype(f32)
            scale = lax.rsqrt(jnp.mean(wide * wide, -1, keepdims=True) + EPS)
            back = scale * (da - wide * (scale * scale * jnp.mean(da * wide, -1, keepdims=True)))
            o_ref[...] = (dy_ref[...].astype(f32) + back).astype(bf16)
            if work:
                assert work.last < 2 * steps
                work.step(2 * pl.program_id(0) + 1)

                @pl.when(pl.program_id(0) == steps - 1)
                def _():
                    work.finish()

        rows = lambda n: pl.BlockSpec((r, n), lambda i: (i, 0))
        matrix = lambda m: pl.BlockSpec((ns, None, share, ff), lambda i: (0, m, 0, 0), pipeline_mode=pl.Buffered(1))
        shape = jax.ShapeDtypeStruct((t, d), bf16)
        return pl.pallas_call(
            kernel,
            grid=(steps,),
            name="by_input",
            in_specs=[rows(a.shape[1]) for a in (*dgs, *dus)] + [matrix(0), matrix(1)] + [rows(d)] * 2 + (work.in_specs if work else []),
            out_specs=[rows(d), work.out_spec] if work else rows(d),
            out_shape=[shape, work.out_shape] if work else shape,
            scratch_shapes=work.scratch if work else [],
            compiler_params=params(collective_id=3, has_side_effects=True) if work else params(),
            cost_estimate=cost(4 * t * d * ff, 4 * t * ff),
        )(*dgs, *dus, pair, pair, h, dy, *(terms or ()))

    def step(x, dy, *weights):
        layers, share, _ = weights[0].shape
        h, dy = x[0], dy[0]
        scattered = lambda term: lax.psum_scatter(term, "s", scatter_dimension=0, tiled=True)
        whole_of = lambda w: lax.all_gather(w, "s", axis=0, tiled=True)

        kept = []
        for number in range(layers):
            gate, up = weights[0][number], weights[1][number]
            if number == 0:
                pair = fetched(gate, up)
            else:
                pair = whole_of(jnp.concatenate([gate, up])).reshape(ns, 2, share, -1)
            wd = whole_of(weights[2][number])
            s1, s2, act, actt, at = gate_up(h, pair)
            kept.append((h, s1, s2, actt, at, pair, wd))
            if number < layers - 1:
                h = down(h, act, wd)
        grads, waiting = [None] * layers, {}
        for number in reversed(range(layers)):
            h, s1, s2, actt, at, pair, wd = kept[number]
            terms = by_down(actt, dy, number == 0)
            if number == 0:
                early, late = FIRST, pair.shape[-1] // WIDE - FIRST
                dg_a, du_a, *terms_a, g_down = by_gate_up(dy, at, wd, s1, s2, 0, early, terms, 5, (1, 4, 5), 1)
                terms_a, waiting = lax.optimization_barrier((terms_a, waiting))
                for n, sums in waiting.items():
                    down_sum, pair_sum = lax.psum(sums, "r")
                    grads[n] = (pair_sum[:share], pair_sum[share:], down_sum)
                dg_b, du_b, *terms_b, g_a = by_gate_up(dy, at, wd, s1, s2, early, late, terms_a, 8, (0, 1, 2, 3, 4, 5), 2)
                dy, g_b = by_input((dg_a, dg_b), (du_a, du_b), pair, h, dy, terms_b)
                g_pair = jnp.concatenate([g_a, g_b], -1)
                grads[number] = (g_pair[:share], g_pair[share:], g_down)
            else:
                down_sum = scattered(terms)
                dg, du, terms = by_gate_up(dy, at, wd, s1, s2, 0, pair.shape[-1] // WIDE)
                dy = by_input((dg,), (du,), pair, h, dy)
                waiting[number] = (down_sum, scattered(terms.reshape(2 * share * ns, -1)))
        return (dy[None], *(jnp.stack([g[i] for g in grads]) for i in range(3)))

    states, cut = P(("rep", "r", "s"), None, None), P(None, "s", None)
    return jax.shard_map(
        step,
        mesh=mesh,
        in_specs=(states, states) + (cut,) * 3,
        out_specs=(states,) + (P("rep", "s", None),) * 3,
        check_vma=False,
    )
```
